512 devices in a mesh: rows: 128 (over y, z, core), rep: 4 (over x).
Axes of the slice: x: 4, y: 8, z: 8, core: 2. Of those that a mesh axis runs over, the one named last changes fastest.
Arguments:
- embed: bfloat16 [65536, 1024], P('rows'), may hold values from -6 to 6
- start: bfloat16 [65536, 128], P('rows'), may hold values from -6 to 6
- links: int32 [128, 128], P('rows'), may hold values from -1 to 3, as said below
Outputs:
- embedding: float32 [65536, 128], P('rows')
The draws below stay inside these ranges and needn't reach their ends.
Inputs may be any that keep to these rules, and one draw needn't show every extreme that they name: `links`: entry [r, s] is -1 (no pair) or a block of owner s; the diagonal is -1; each row has at most 96 entries other than -1, and some row has exactly 96.
All inputs are finite; a program needn't handle non-finite values.
Results may differ from the reference program's by a relative error of at most 0.012.
Values may be sent and summed in bfloat16 or wider, within the bound.
No kernel may reach another device: no remote copies, remote signals or barrier semaphores. Data moves between devices by JAX's collectives and lax.ppermute only.
A program may use at most 128 MiB of HBM per device.

```python
import math
import jax
import jax.numpy as jnp
from jax import lax

D = 1024
K = 128
BLOCK = 128
BLOCKS_DEV = 4
ITERS = 2
POINTS = 65536
LINK_MAX = 96
N_ROWS = 128


def draw_links(key, part):
    base_key = jax.random.fold_in(key, 11)
    level_key, busy_key, order_key, block_key = jax.random.split(base_key, 4)
    owner_ids = jnp.arange(N_ROWS)
    levels = jax.random.randint(level_key, (N_ROWS,), 0, 2)
    counts = jnp.maximum(jnp.right_shift(jnp.full((N_ROWS,), LINK_MAX, jnp.int32), levels), 1)
    busiest = jax.random.randint(busy_key, (), 0, N_ROWS)
    counts = jnp.where(owner_ids == busiest, LINK_MAX, counts)
    row_keys = jax.random.split(order_key, N_ROWS)
    shuffles = jax.vmap(lambda row_key: jax.random.permutation(row_key, N_ROWS))(row_keys)
    rank_order = jnp.argsort(shuffles, axis=1, stable=True)
    self_rank = jnp.sum(jnp.where(owner_ids[:, None] == owner_ids[None, :], rank_order, 0), axis=1)
    other_rank = rank_order - (rank_order > self_rank[:, None]).astype(jnp.int32)
    is_self = owner_ids[:, None] == owner_ids[None, :]
    alive_link = jnp.logical_and(other_rank < counts[:, None], jnp.logical_not(is_self))
    chosen = jax.random.randint(block_key, (N_ROWS, N_ROWS), 0, BLOCKS_DEV)
    return jnp.where(alive_link, chosen, -1).astype(jnp.int32)


def block_scale(rng, shape, shards, low, top_value):
    def one(axis_at, shards_of):
        draws = jax.random.uniform(jax.random.fold_in(jax.random.fold_in(rng, 6), axis_at), (shards_of,), jnp.float32, low / len(shards), top_value / len(shards))
        return jnp.repeat(jnp.exp(draws), shape[axis_at] // shards_of).reshape((-1,) + (1,) * (len(shape) - axis_at - 1))

    loudness = one(*shards[0])
    for cut in shards[1:]:
        loudness = loudness * one(*cut)
    return loudness


def gaussian(rng, dims, width, bound, cuts=(), held_as=jnp.bfloat16):
    values = width * jax.random.normal(rng, dims, jnp.float32)
    if cuts:
        values = values * block_scale(rng, dims, cuts, -0.22, 0.18)
    return jnp.clip(values, -bound, bound).astype(held_as)


def setup_inputs(seed: int = 0) -> dict:
    keys = jax.random.split(jax.random.key(seed), 4)
    embed = gaussian(keys[0], (POINTS, D), 1.0, 6.0, ((0, 128),))
    start = gaussian(keys[1], (POINTS, K), 1.0, 6.0, ((0, 128),))
    links = draw_links(jax.random.fold_in(keys[3], 71), 0)
    return {"embed": embed, "start": start, "links": links}


EPSILON = 1e-06

def row_scale(rows):
    values = rows.astype(jnp.float32)
    return lax.rsqrt(lax.optimization_barrier(jnp.mean(values * values, axis=-1)) + EPSILON)

def orthonormal(result, gram_matrix):
    lower_factor = jnp.linalg.cholesky(gram_matrix)
    return lax.linalg.triangular_solve(lower_factor, result, left_side=False, lower=True, transpose_a=True)

def reference(embed, start, links):
    feature_count = embed.shape[1]
    comp_count = start.shape[1]
    spread = 2.0 / math.sqrt(feature_count)
    owners = links.shape[0]
    slab_rows = embed.shape[0] // owners
    blocks = slab_rows // BLOCK
    scales = row_scale(embed).reshape(owners, slab_rows)
    slabs = embed.reshape(owners, slab_rows, feature_count)
    block_rows = embed.reshape(owners, blocks, BLOCK, feature_count)
    block_scales = scales.reshape(owners, blocks, BLOCK)
    self_mask = jnp.arange(slab_rows)[:, None] == jnp.arange(slab_rows)[None, :]

    def owner_tiles(owner_index):
        link_row = lax.dynamic_index_in_dim(links, owner_index, 0, keepdims=False)
        slot_order = jnp.argsort((link_row < 0).astype(jnp.int32), stable=True)[:LINK_MAX].astype(jnp.int32)
        chosen = jnp.clip(link_row[slot_order], 0, blocks - 1).astype(jnp.int32)
        alive_slot = (link_row[slot_order] >= 0).astype(jnp.float32)
        pieces = block_rows[slot_order, chosen].reshape(-1, feature_count)
        piece_scale = block_scales[slot_order, chosen]
        own_rows = lax.dynamic_index_in_dim(slabs, owner_index, 0, keepdims=False)
        own_scale = lax.dynamic_index_in_dim(scales, owner_index, 0, keepdims=False)
        products_in = jnp.dot(pieces.astype(jnp.float32), own_rows.T.astype(jnp.float32), preferred_element_type=jnp.float32).reshape(LINK_MAX, BLOCK, slab_rows)
        exponent = spread * products_in * piece_scale[:, :, None] * own_scale[None, None, :]
        pair_tiles = (jnp.exp(exponent) * alive_slot[:, None, None]).astype(jnp.bfloat16)
        self_products = jnp.dot(own_rows.astype(jnp.float32), own_rows.T.astype(jnp.float32), preferred_element_type=jnp.float32)
        self_exponent = spread * self_products * own_scale[:, None] * own_scale[None, :]
        square = jnp.where(self_mask, 0.0, jnp.exp(self_exponent)).astype(jnp.bfloat16)
        return (slot_order, chosen, pair_tiles, square)

    def degree_step(summed_all, owner_index):
        slot_order, chosen, pair_tiles, square = owner_tiles(owner_index)
        own_sums = lax.optimization_barrier(jnp.sum(pair_tiles, axis=(0, 1), dtype=jnp.float32)) + lax.optimization_barrier(jnp.sum(square, axis=0, dtype=jnp.float32))
        back_sums = lax.optimization_barrier(jnp.sum(pair_tiles, axis=2, dtype=jnp.float32))
        summed_all = summed_all.at[owner_index].add(own_sums.reshape(blocks, BLOCK))
        summed_all = summed_all.at[slot_order, chosen].add(back_sums)
        return (summed_all, None)
    owner_ids = jnp.arange(owners, dtype=jnp.int32)
    degree = lax.scan(degree_step, jnp.zeros((owners, blocks, BLOCK), jnp.float32), owner_ids)[0].reshape(-1)
    inv_root = lax.rsqrt(degree)
    current = start.astype(jnp.float32)
    for turn_index in range(ITERS):
        scaled = (current * inv_root[:, None]).astype(jnp.bfloat16)
        scaled_slabs = scaled.reshape(owners, slab_rows, comp_count)
        scaled_blocks = scaled.reshape(owners, blocks, BLOCK, comp_count)

        def product_step(summed_all, owner_index):
            slot_order, chosen, pair_tiles, square = owner_tiles(owner_index)
            own_rows = lax.dynamic_index_in_dim(scaled_slabs, owner_index, 0, keepdims=False)
            fetched = scaled_blocks[slot_order, chosen].reshape(-1, comp_count)
            flat_rows = pair_tiles.reshape(-1, slab_rows)
            forward = jnp.dot(flat_rows.T.astype(jnp.float32), fetched.astype(jnp.float32), preferred_element_type=jnp.float32)
            forward = forward + jnp.dot(square.astype(jnp.float32), own_rows.astype(jnp.float32), preferred_element_type=jnp.float32)
            back_sums = jnp.dot(flat_rows.astype(jnp.float32), own_rows.astype(jnp.float32), preferred_element_type=jnp.float32).reshape(LINK_MAX, BLOCK, comp_count)
            summed_all = summed_all.at[owner_index].add(forward.reshape(blocks, BLOCK, comp_count))
            summed_all = summed_all.at[slot_order, chosen].add(back_sums)
            return (summed_all, None)
        zeros_all = jnp.zeros((owners, blocks, BLOCK, comp_count), jnp.float32)
        summed_all = lax.scan(product_step, zeros_all, owner_ids)[0].reshape(-1, comp_count)
        result = summed_all * inv_root[:, None]
        gram_matrix = jnp.dot(result.T, result, precision=lax.Precision.HIGHEST)
        current = orthonormal(result, gram_matrix)
    return current * math.sqrt(embed.shape[0])
```

```python
import math

import jax
import jax.numpy as jnp
from jax import lax
from jax.sharding import Mesh, PartitionSpec as P

BLOCK = 128
BLOCKS_DEV = 4
ITERS = 2
EPSILON = 1e-06
ROWS = ("y", "z", "c")


def row_scale(rows):
    values = rows.astype(jnp.float32)
    return lax.rsqrt(jnp.mean(values * values, axis=-1) + EPSILON)


def orthonormal(result, gram_matrix):
    lower_factor = jnp.linalg.cholesky(gram_matrix)
    return lax.linalg.triangular_solve(
        lower_factor, result, left_side=False, lower=True, transpose_a=True
    )


def pair_counts(table, y_count, z_count):
    y, z, c, x = (lax.axis_index(name) for name in ("y", "z", "c", "x"))
    by_place = table.reshape(y_count, z_count, 2, y_count, z_count, 2)
    ahead = by_place[y, :, c][:, :, z]
    back = by_place[:, z, :, y, :, c]
    back = jnp.transpose(back, (2, 0, 1))
    blocks = jnp.arange(BLOCKS_DEV)
    same = (
        (jnp.arange(z_count)[:, None, None] == z)
        & (jnp.arange(y_count)[None, :, None] == y)
        & (jnp.arange(2)[None, None, :] == c)
    )
    counts = (
        (ahead == x).astype(jnp.float32)[:, None]
        + (back[:, None] == blocks[None, :, None, None]).astype(jnp.float32)
        + same.astype(jnp.float32)[:, None]
    )
    return counts.reshape(z_count * BLOCKS_DEV, y_count * 2)


def on_device(embed, start, links):
    y_count, z_count = lax.axis_size("y"), lax.axis_size("z")
    y, z, c, x = (lax.axis_index(name) for name in ("y", "z", "c", "x"))
    slab_rows, feature_count = embed.shape
    points = slab_rows * y_count * z_count * 2
    spread = 2.0 / math.sqrt(feature_count)
    highest = lax.Precision.HIGHEST

    own = lax.dynamic_slice_in_dim(embed, x * BLOCK, BLOCK, 0)
    table = lax.all_gather(links, ROWS, axis=0, tiled=True)
    cols = lax.all_gather(own, ("y", "c"), axis=0, tiled=True)
    rows = lax.all_gather(own, ("z", "x"), axis=0, tiled=True)
    counts = pair_counts(table, y_count, z_count)
    products = lax.dot_general(
        rows, cols, (((1,), (1,)), ((), ())), preferred_element_type=jnp.float32
    )
    exponent = spread * products * row_scale(rows)[:, None] * row_scale(cols)[None, :]
    row_ids = jnp.arange(rows.shape[0])[:, None]
    col_ids = jnp.arange(cols.shape[0])[None, :]
    offset = (z * BLOCKS_DEV + x) * BLOCK - (y * 2 + c) * BLOCK
    on_diagonal = (row_ids - col_ids == offset) & (col_ids // BLOCK == y * 2 + c)
    weight = jnp.repeat(jnp.repeat(counts, BLOCK, axis=0), BLOCK, axis=1)
    weight = jnp.where(on_diagonal, 0.0, weight)
    tile = (jnp.exp(exponent) * weight).astype(jnp.bfloat16)
    sums = jnp.sum(tile, axis=1, dtype=jnp.float32).reshape(-1, BLOCK)
    got = lax.all_to_all(sums, ("z", "x"), split_axis=0, concat_axis=0, tiled=True)
    inv_root = lax.rsqrt(jnp.sum(got, axis=0))[:, None]

    current = lax.dynamic_slice_in_dim(start, x * BLOCK, BLOCK, 0).astype(jnp.float32)
    for turn in range(ITERS):
        scaled = (current * inv_root).astype(jnp.bfloat16)
        fetched = lax.all_gather(scaled, ("y", "c"), axis=0, tiled=True)
        part = jnp.dot(tile, fetched, preferred_element_type=jnp.float32)
        total = lax.psum_scatter(part, ("z", "x"), scatter_dimension=0, tiled=True)
        result = total * inv_root
        gram = lax.psum(jnp.dot(result.T, result, precision=highest), ("y", "z", "c", "x"))
        if turn == ITERS - 1:
            result = lax.all_gather(result, "x", axis=0, tiled=True)
        current = orthonormal(result, gram)
    return current * math.sqrt(points)


def solution(mesh):
    owners, reps = mesh.devices.shape
    side = math.isqrt(owners // 2)
    fine = Mesh(mesh.devices.reshape(side, side, 2, reps), ("y", "z", "c", "x"))
    return jax.shard_map(
        on_device,
        mesh=fine,
        in_specs=(P(ROWS, None), P(ROWS, None), P(ROWS, None)),
        out_specs=P(ROWS, None),
        check_vma=False,
    )
```

```python
import functools
import math

import jax
import jax.numpy as jnp
from jax import lax
from jax.experimental import pallas as pl
from jax.experimental.pallas import tpu as pltpu
from jax.sharding import Mesh, PartitionSpec as P

BLOCK = 128
PAIR = 2 * BLOCK
EXTRA = 8
ITERS = 2
EPSILON = 1e-06
ROWS = ("y", "z", "c")
ROW_GROUP = ("z", "xb")
COL_GROUP = ("y", "c", "xa")


def from_everyone(shard, axes):
    copies = jnp.broadcast_to(shard, (lax.axis_size(axes), *shard.shape))
    return lax.all_to_all(copies, axes, split_axis=0, concat_axis=0, tiled=True)


def total_of(shard, axes):
    return jnp.sum(from_everyone(shard, axes), axis=0)


def gram_total(gram):
    wide = ("z", "xa", "xb")
    parts = gram.reshape(lax.axis_size(wide), -1, gram.shape[1])
    share = jnp.sum(lax.all_to_all(parts, wide, split_axis=0, concat_axis=0, tiled=True), axis=0)
    share = total_of(share, ("y", "c"))
    return from_everyone(share, wide).reshape(gram.shape)


def orthonormal(result, gram_matrix):
    lower_factor = jnp.linalg.cholesky(gram_matrix)
    return lax.linalg.triangular_solve(
        lower_factor, result, left_side=False, lower=True, transpose_a=True
    )


def ring(own, axis):
    size = lax.axis_size(axis)
    onward = [(i, (i + 1) % size) for i in range(size)]
    backward = [(i, (i - 1) % size) for i in range(size)]
    got = {0: [(own, 0)]}
    ahead = behind = own
    for step in range(1, size // 2):
        ahead = lax.ppermute(ahead, axis, onward)
        behind = lax.ppermute(behind, axis, backward)
        got[size - step] = [(ahead, 0)]
        got[step] = [(behind, 0)]
    top = lax.ppermute(ahead[:BLOCK], axis, onward)
    rest = lax.ppermute(behind[BLOCK:], axis, backward)
    got[size // 2] = [(top, 0), (rest, BLOCK)]
    return got


def tile_kernel(plan, sizes, ids, *refs):
    y_count, z_count, features, comps = sizes
    row_plan, col_plan = plan
    count = len(row_plan) + len(col_plan)
    pieces, (w_out, sums_out, v_out) = refs[:count], refs[count : count + 3]
    rows_v, cols_v, start_v, row_links, col_links, weight, w_v, sems, out_sems = refs[count + 3 :]
    y, z, c, xa, xb = (ids[i] for i in range(5))
    row_owners, col_owners = z_count, 2 * y_count
    copies = []

    def copy(src, dst):
        made = pltpu.make_async_copy(src, dst, sems.at[len(copies)])
        made.start()
        copies.append(made)

    for ref, (k, first, height) in zip(pieces, row_plan):
        owner = lax.rem(z + k, z_count)
        body = min(height, PAIR - first)
        at = pl.multiple_of(owner * PAIR + first, BLOCK)
        copy(ref.at[pl.ds(0, body)], rows_v.at[pl.ds(at, body)])
        if first + height > PAIR:
            copy(ref.at[pl.ds(body, EXTRA), pl.ds(0, BLOCK)], row_links.at[owner])
    for ref, (k, other, first, height) in zip(pieces[len(row_plan) :], col_plan):
        owner = lax.rem(y + k, y_count) * 2 + (1 - c if other else c)
        body = min(height, PAIR - first)
        at = pl.multiple_of(owner * PAIR + first, BLOCK)
        copy(ref.at[pl.ds(0, body), pl.ds(0, features)], cols_v.at[pl.ds(at, body)])
        copy(ref.at[pl.ds(0, body), pl.ds(features, comps)], start_v.at[pl.ds(at, body)])
        if first + height > PAIR:
            copy(ref.at[pl.ds(body, EXTRA), pl.ds(0, BLOCK)], col_links.at[owner])
    for made in copies:
        made.wait()
    v_copy = pltpu.make_async_copy(start_v, v_out, out_sems.at[col_owners])
    v_copy.start()

    width = col_owners * PAIR
    lane = lax.broadcasted_iota(jnp.int32, (BLOCK, width), 1)
    place = lax.broadcasted_iota(jnp.int32, (BLOCK, width), 0)
    lane_owner = lane // PAIR
    lane_slab = ((lane_owner // 2) * z_count + z) * 2 + lane_owner % 2
    select = (place == lane_slab).astype(jnp.bfloat16)
    ahead_rows = jnp.concatenate([row_links[k][0:1] for k in range(row_owners)], axis=0)
    ahead = jnp.dot(ahead_rows, select, preferred_element_type=jnp.float32)
    spread_to = (place[:col_owners] == lane_owner[:col_owners]).astype(jnp.bfloat16)
    back_rows = jnp.concatenate([col_links[k][0:1] for k in range(col_owners)], axis=0)
    spread_back = lax.dot_general(
        back_rows, spread_to, (((0,), (0,)), ((), ())), preferred_element_type=jnp.float32
    ).astype(jnp.bfloat16)
    row_slab = (y * z_count + lax.broadcasted_iota(jnp.int32, (row_owners, BLOCK), 0)) * 2 + c
    row_pick = lax.broadcasted_iota(jnp.int32, (row_owners, BLOCK), 1) == row_slab
    back = jnp.dot(row_pick.astype(jnp.bfloat16), spread_back, preferred_element_type=jnp.float32)
    col_block = (xb + 2 * ((lane[:row_owners] // BLOCK) % 2)).astype(jnp.float32)
    same = (lane_owner[:row_owners] == y * 2 + c) & (place[:row_owners] == z)
    base = (ahead == col_block).astype(jnp.float32) + same.astype(jnp.float32)
    for half in range(2):
        row_block = (2 * xa + half).astype(jnp.float32)
        weight[half] = base + (back == row_block).astype(jnp.float32)

    factor = 2.0 / math.sqrt(features) * math.log2(math.e)

    def scale_of(values):
        wide = values.astype(jnp.float32)
        mean = jnp.sum(wide * wide, axis=-1, keepdims=True) * (1.0 / features)
        return lax.rsqrt(mean + EPSILON)

    row_scales = [
        scale_of(rows_v[pl.ds(i * PAIR, PAIR)]) * factor for i in range(row_owners)
    ]
    eye = lax.broadcasted_iota(jnp.int32, (BLOCK, BLOCK), 0) == lax.broadcasted_iota(
        jnp.int32, (BLOCK, BLOCK), 1
    )

    def out_copy(j):
        where = pl.ds(pl.multiple_of(j * PAIR, PAIR), PAIR)
        return pltpu.make_async_copy(w_v.at[:, where], w_out.at[:, where], out_sems.at[j])

    own_col = y * 2 + c

    def column(j, carry):
        at = pl.multiple_of(j * PAIR, PAIR)
        part = cols_v[pl.ds(at, PAIR)]
        scale = jnp.transpose(jnp.broadcast_to(scale_of(part), (PAIR, BLOCK)))[0:1]
        sums = [jnp.zeros((1, BLOCK), jnp.float32) for _ in range(2)]
        for i in range(row_owners):
            products = lax.dot_general(
                rows_v[i * PAIR : (i + 1) * PAIR],
                part,
                (((1,), (1,)), ((), ())),
                preferred_element_type=jnp.float32,
            )
            values = jnp.exp2(products * row_scales[i] * scale)
            for half in range(2):
                counts = weight[half, pl.ds(i, 1), pl.ds(at, PAIR)]
                for side in range(2):
                    block = values[half * BLOCK : (half + 1) * BLOCK, side * BLOCK : (side + 1) * BLOCK]
                    block = block * counts[:, side * BLOCK : (side + 1) * BLOCK]
                    mine = (j == own_col) & (z == i) & (xb == half) & (xa == side)
                    block = jnp.where(eye & mine, 0.0, block).astype(jnp.bfloat16)
                    w_v[
                        pl.ds(i * PAIR + half * BLOCK, BLOCK),
                        pl.ds(pl.multiple_of(at + side * BLOCK, BLOCK), BLOCK),
                    ] = block
                    sums[side] += jnp.sum(block.astype(jnp.float32), axis=0, keepdims=True)
        sums_out[:, pl.ds(at, PAIR)] = jnp.concatenate(sums, axis=1)
        out_copy(j).start()
        return carry

    lax.fori_loop(0, col_owners, column, 0)

    def drain(j, carry):
        out_copy(j).wait()
        return carry

    lax.fori_loop(0, col_owners, drain, 0)
    v_copy.wait()


def build_tile(row_pieces, col_pieces, ids, features, comps):
    y_count, z_count = lax.axis_size("y"), lax.axis_size("z")
    row_plan, col_plan, operands = [], [], []
    for k in sorted(row_pieces):
        for piece, first in row_pieces[k]:
            row_plan.append((k, first, piece.shape[0]))
            operands.append(piece)
    for k, other in sorted(col_pieces):
        for piece, first in col_pieces[k, other]:
            col_plan.append((k, other, first, piece.shape[0]))
            operands.append(piece)
    height, width = z_count * PAIR, 2 * y_count * PAIR
    copies = 2 * len(row_plan) + 3 * len(col_plan)
    kernel = functools.partial(
        tile_kernel, (row_plan, col_plan), (y_count, z_count, features, comps)
    )
    return pl.pallas_call(
        kernel,
        out_shape=(
            jax.ShapeDtypeStruct((height, width), jnp.bfloat16),
            jax.ShapeDtypeStruct((1, width), jnp.float32),
            jax.ShapeDtypeStruct((width, comps), jnp.bfloat16),
        ),
        in_specs=[pl.BlockSpec(memory_space=pltpu.SMEM)]
        + [pl.BlockSpec(memory_space=pl.ANY)] * len(operands),
        out_specs=(
            pl.BlockSpec(memory_space=pl.ANY),
            pl.BlockSpec(memory_space=pltpu.VMEM),
            pl.BlockSpec(memory_space=pl.ANY),
        ),
        scratch_shapes=[
            pltpu.VMEM((height, features), jnp.bfloat16),
            pltpu.VMEM((width, features), jnp.bfloat16),
            pltpu.VMEM((width, comps), jnp.bfloat16),
            pltpu.VMEM((z_count, EXTRA, BLOCK), jnp.bfloat16),
            pltpu.VMEM((2 * y_count, EXTRA, BLOCK), jnp.bfloat16),
            pltpu.VMEM((2, z_count, width), jnp.float32),
            pltpu.VMEM((height, width), jnp.bfloat16),
            pltpu.SemaphoreType.DMA((copies,)),
            pltpu.SemaphoreType.DMA((2 * y_count + 1,)),
        ],
        compiler_params=pltpu.CompilerParams(vmem_limit_bytes=58 * 1024 * 1024),
        cost_estimate=pl.CostEstimate(
            flops=2 * height * width * features,
            bytes_accessed=2 * (height + width) * features + 2 * height * width,
            transcendentals=height * width,
        ),
        name="affinity_tile",
    )(ids, *operands)


def on_device(embed, start, links):
    slab_rows, features = embed.shape
    comps = start.shape[1]
    y_count, z_count = lax.axis_size("y"), lax.axis_size("z")
    y, z, c, xa, xb = (lax.axis_index(name) for name in ("y", "z", "c", "xa", "xb"))
    points = slab_rows * 2 * y_count * z_count
    highest = lax.Precision.HIGHEST

    note = jnp.pad(links.astype(jnp.bfloat16), ((0, EXTRA - 1), (0, BLOCK - links.shape[1])))
    row_own = lax.dynamic_slice_in_dim(embed, xa * PAIR, PAIR, 0)
    row_own = jnp.concatenate(
        [row_own, jnp.pad(note, ((0, 0), (0, features - BLOCK)))], axis=0
    )

    def blocks_of(values):
        shaped = values.reshape(2, 2, BLOCK, values.shape[1])
        return lax.dynamic_index_in_dim(shaped, xb, 1, keepdims=False).reshape(PAIR, -1)

    col_own = jnp.concatenate([blocks_of(embed), blocks_of(start)], axis=1)
    col_own = jnp.concatenate(
        [col_own, jnp.pad(note, ((0, 0), (0, features + comps - BLOCK)))], axis=0
    )
    row_pieces = ring(row_own, "z")
    swap = [(0, 1), (1, 0)]
    col_pieces = {}
    for k, held in ring(col_own, "y").items():
        col_pieces[k, 0] = held
        col_pieces[k, 1] = [(lax.ppermute(piece, "c", swap), first) for piece, first in held]
    ids = jnp.stack([y, z, c, xa, xb]).astype(jnp.int32)
    tile, sums, fetched_start = build_tile(row_pieces, col_pieces, ids, features, comps)

    inv_root_cols = lax.rsqrt(total_of(sums, COL_GROUP))[0]
    own_at = (y * 2 + c) * PAIR + xa * BLOCK
    inv_root = lax.dynamic_slice_in_dim(inv_root_cols, own_at, BLOCK, 0)[:, None]
    fetched = (fetched_start.astype(jnp.float32) * inv_root_cols[:, None]).astype(jnp.bfloat16)
    for turn in range(ITERS):
        part = jnp.dot(tile, fetched, preferred_element_type=jnp.float32).astype(jnp.bfloat16)
        parts = part.reshape(-1, BLOCK, comps)
        got = lax.all_to_all(parts, ROW_GROUP, split_axis=0, concat_axis=0, tiled=True)
        result = jnp.sum(got.astype(jnp.float32), axis=0) * inv_root
        gram = gram_total(jnp.dot(result.T, result, precision=highest))
        if turn == ITERS - 1:
            result = from_everyone(result, ("xa", "xb")).reshape(slab_rows, comps)
            return orthonormal(result, gram) * math.sqrt(points)
        current = orthonormal(result, gram)
        scaled = (current * inv_root).astype(jnp.bfloat16)
        fetched = from_everyone(scaled, COL_GROUP).reshape(-1, comps)


def solution(mesh):
    owners, reps = mesh.devices.shape
    side = math.isqrt(owners // 2)
    fine = Mesh(mesh.devices.reshape(side, side, 2, 2, reps // 2), ("y", "z", "c", "xa", "xb"))
    return jax.shard_map(
        on_device,
        mesh=fine,
        in_specs=(P(ROWS, None), P(ROWS, None), P(ROWS, None)),
        out_specs=P(ROWS, None),
        check_vma=False,
    )
```

```python
import functools
import math

import jax
import jax.numpy as jnp
from jax import lax
from jax.experimental import pallas as pl
from jax.experimental.pallas import tpu as pltpu
from jax.sharding import Mesh, PartitionSpec as P

BLOCK = 128
PAIR = 2 * BLOCK
EXTRA = 8
GROUP = 8
ITERS = 2
EPSILON = 1e-06
ROWS = ("y", "z", "c")
ROW_GROUP = ("z", "xb")
COL_GROUP = ("y", "c", "xa")


def from_everyone(shard, axes):
    copies = jnp.broadcast_to(shard, (lax.axis_size(axes), *shard.shape))
    return lax.all_to_all(copies, axes, split_axis=0, concat_axis=0, tiled=True)


def total_of(shard, axes):
    return jnp.sum(from_everyone(shard, axes), axis=0)


def gram_total(gram):
    parts = gram.reshape(lax.axis_size(ROW_GROUP), -1, gram.shape[1])
    share = jnp.sum(
        lax.all_to_all(parts, ROW_GROUP, split_axis=0, concat_axis=0, tiled=True), axis=0
    )
    share = total_of(share, COL_GROUP)
    return from_everyone(share, ROW_GROUP).reshape(gram.shape)


def inverse_factor_kernel(gram_ref, out_ref):
    size = gram_ref.shape[0]
    count = size // GROUP
    diag = lax.broadcasted_iota(jnp.int32, (GROUP, size), 1) - lax.broadcasted_iota(
        jnp.int32, (GROUP, size), 0
    )
    sub = lax.broadcasted_iota(jnp.int32, (GROUP, size), 0)
    left = [gram_ref[g * GROUP : (g + 1) * GROUP] for g in range(count)]
    right = [(diag == g * GROUP).astype(jnp.float32) for g in range(count)]
    pivots = [None] * count

    def wide(column):
        return jnp.broadcast_to(column, (GROUP, size))

    def tall(row):
        return jnp.broadcast_to(row, (GROUP, size))

    for k in range(0, size, 2):
        home, at = divmod(k, GROUP)
        here = slice(at, at + 1)
        after = slice(at + 1, at + 2)
        first = [wide(left[g][:, k : k + 1]) for g in range(home, count)]
        second = [wide(left[g][:, k + 1 : k + 2]) for g in range(home, count)]
        a = tall(first[0][here])
        b = tall(first[0][after])
        d = tall(second[0][after])
        ratio = b / a
        rest = d - b * ratio
        inv_a, inv_rest = 1.0 / a, 1.0 / rest
        row_left, row_right = tall(left[home][here]), tall(right[home][here])
        next_left = tall(left[home][after]) - ratio * row_left
        next_right = tall(right[home][after]) - ratio * row_right
        for g in range(home, count):
            f = first[g - home] * inv_a
            h = (second[g - home] - first[g - home] * ratio) * inv_rest
            if g == home:
                mine = jnp.where(sub == at, a, jnp.where(sub == at + 1, rest, 0.0))
                pivots[g] = mine if pivots[g] is None else pivots[g] + mine
                f = jnp.where(sub > at, f, 0.0)
                h = jnp.where(sub > at + 1, h, 0.0)
            if g > home or at + 2 < GROUP:
                left[g] = left[g] - f * row_left - h * next_left
            right[g] = right[g] - f * row_right - h * next_right
    for g in range(count):
        out_ref[g * GROUP : (g + 1) * GROUP] = right[g] * lax.rsqrt(pivots[g])


def inverse_factor(gram):
    return pl.pallas_call(
        inverse_factor_kernel,
        out_shape=jax.ShapeDtypeStruct(gram.shape, jnp.float32),
        in_specs=[pl.BlockSpec(memory_space=pltpu.VMEM)],
        out_specs=pl.BlockSpec(memory_space=pltpu.VMEM),
        name="inverse_factor",
    )(gram)


def orthonormal(result, gram_matrix):
    inverse = inverse_factor(gram_matrix)
    return lax.dot_general(
        result, inverse, (((1,), (1,)), ((), ())), precision=lax.Precision.HIGHEST
    )


def exchange(row_own, col_own):
    row_size, col_size = lax.axis_size("z"), lax.axis_size("y")
    assert row_size == col_size
    size = row_size
    onward = [(i, (i + 1) % size) for i in range(size)]
    backward = [(i, (i - 1) % size) for i in range(size)]
    height = row_own.shape[0]
    rows = [(row_own, 0, 0, 0, height)]
    cols = [(col_own, 0, 0, 0, False, height)]
    waiting = [(0, 0, col_own)]
    swaps = []

    def swap(batch):
        joined = jnp.concatenate([piece for _, _, piece in batch], axis=0)
        other = lax.ppermute(joined, "c", [(0, 1), (1, 0)])
        at = 0
        for place, first, piece in batch:
            swaps.append((place, first, at, piece.shape[0]))
            at += piece.shape[0]
        return other

    others = []
    held = (row_own, row_own, col_own, col_own)
    for step in range(1, size // 2):
        row_a, row_b, col_a, col_b = held
        held = (
            lax.ppermute(row_a, "z", onward),
            lax.ppermute(row_b, "z", backward),
            lax.ppermute(col_a, "y", onward),
            lax.ppermute(col_b, "y", backward),
        )
        if step > 1:
            others.append((swap(waiting), len(waiting)))
            waiting = []
        if len(others) > 1:
            tied = lax.optimization_barrier((held, others[-2][0]))
            held, others[-2] = tied[0], (tied[1], others[-2][1])
        else:
            held = lax.optimization_barrier(held)
        for piece, place in zip(held[:2], (size - step, step)):
            rows.append((piece, 0, place, 0, height))
        for piece, place in zip(held[2:], (size - step, step)):
            cols.append((piece, 0, place, 0, False, height))
            waiting.append((place, 0, piece))
    row_a, row_b, col_a, col_b = held
    halves = (
        lax.ppermute(col_a[:BLOCK], "y", onward),
        lax.ppermute(col_b[BLOCK:], "y", backward),
        lax.ppermute(row_a[:BLOCK], "z", onward),
        lax.ppermute(row_b[BLOCK:], "z", backward),
    )
    others.append((swap(waiting), len(waiting)))
    waiting = []
    far = size // 2
    for piece, first in zip(halves[:2], (0, BLOCK)):
        cols.append((piece, 0, far, first, False, piece.shape[0]))
        waiting.append((far, first, piece))
    for piece, first in zip(halves[2:], (0, BLOCK)):
        rows.append((piece, 0, far, first, piece.shape[0]))
    others.append((swap(waiting), len(waiting)))
    done = 0
    for other, count in others:
        for place, first, at, tall in swaps[done : done + count]:
            cols.append((other, at, place, first, True, tall))
        done += count
    return rows, cols


def tile_kernel(plan, sizes, ids, *refs):
    y_count, z_count, features, comps = sizes
    count, row_plan, col_plan = plan
    pieces, (w_out, sums_out, v_out) = refs[:count], refs[count : count + 3]
    rows_v, cols_v, start_v, row_links, col_links, weight, w_v, sems, out_sems = refs[count + 3 :]
    y, z, c, xa, xb = (ids[i] for i in range(5))
    row_owners, col_owners = z_count, 2 * y_count
    copies = []

    def copy(src, dst):
        made = pltpu.make_async_copy(src, dst, sems.at[len(copies)])
        made.start()
        copies.append(made)

    for slot, source, k, first, height in row_plan:
        ref = pieces[slot]
        owner = lax.rem(z + k, z_count)
        body = min(height, PAIR - first)
        at = pl.multiple_of(owner * PAIR + first, BLOCK)
        copy(ref.at[pl.ds(source, body)], rows_v.at[pl.ds(at, body)])
        if first + height > PAIR:
            copy(ref.at[pl.ds(source + body, EXTRA), pl.ds(0, BLOCK)], row_links.at[owner])
    for slot, source, k, first, other, height in col_plan:
        ref = pieces[slot]
        owner = lax.rem(y + k, y_count) * 2 + (1 - c if other else c)
        body = min(height, PAIR - first)
        at = pl.multiple_of(owner * PAIR + first, BLOCK)
        from_rows = pl.ds(source, body)
        copy(ref.at[from_rows, pl.ds(0, features)], cols_v.at[pl.ds(at, body)])
        copy(ref.at[from_rows, pl.ds(features, comps)], start_v.at[pl.ds(at, body)])
        if first + height > PAIR:
            copy(ref.at[pl.ds(source + body, EXTRA), pl.ds(0, BLOCK)], col_links.at[owner])
    for made in copies:
        made.wait()
    v_copy = pltpu.make_async_copy(start_v, v_out, out_sems.at[col_owners])
    v_copy.start()

    width = col_owners * PAIR
    lane = lax.broadcasted_iota(jnp.int32, (BLOCK, width), 1)
    place = lax.broadcasted_iota(jnp.int32, (BLOCK, width), 0)
    lane_owner = lane // PAIR
    lane_slab = ((lane_owner // 2) * z_count + z) * 2 + lane_owner % 2
    select = (place == lane_slab).astype(jnp.bfloat16)
    ahead_rows = jnp.concatenate([row_links[k][0:1] for k in range(row_owners)], axis=0)
    ahead = jnp.dot(ahead_rows, select, preferred_element_type=jnp.float32)
    spread_to = (place[:col_owners] == lane_owner[:col_owners]).astype(jnp.bfloat16)
    back_rows = jnp.concatenate([col_links[k][0:1] for k in range(col_owners)], axis=0)
    spread_back = lax.dot_general(
        back_rows, spread_to, (((0,), (0,)), ((), ())), preferred_element_type=jnp.float32
    ).astype(jnp.bfloat16)
    row_slab = (y * z_count + lax.broadcasted_iota(jnp.int32, (row_owners, BLOCK), 0)) * 2 + c
    row_pick = lax.broadcasted_iota(jnp.int32, (row_owners, BLOCK), 1) == row_slab
    back = jnp.dot(row_pick.astype(jnp.bfloat16), spread_back, preferred_element_type=jnp.float32)
    col_block = (xb + 2 * ((lane[:row_owners] // BLOCK) % 2)).astype(jnp.float32)
    same = (lane_owner[:row_owners] == y * 2 + c) & (place[:row_owners] == z)
    base = (ahead == col_block).astype(jnp.float32) + same.astype(jnp.float32)
    for half in range(2):
        row_block = (2 * xa + half).astype(jnp.float32)
        weight[half] = base + (back == row_block).astype(jnp.float32)

    factor = 2.0 / math.sqrt(features) * math.log2(math.e)

    def scale_of(values):
        wide = values.astype(jnp.float32)
        mean = jnp.sum(wide * wide, axis=-1, keepdims=True) * (1.0 / features)
        return lax.rsqrt(mean + EPSILON)

    row_scales = [
        scale_of(rows_v[pl.ds(i * PAIR, PAIR)]) * factor for i in range(row_owners)
    ]
    eye = lax.broadcasted_iota(jnp.int32, (BLOCK, BLOCK), 0) == lax.broadcasted_iota(
        jnp.int32, (BLOCK, BLOCK), 1
    )

    def out_copy(j):
        where = pl.ds(pl.multiple_of(j * PAIR, PAIR), PAIR)
        return pltpu.make_async_copy(w_v.at[:, where], w_out.at[:, where], out_sems.at[j])

    own_col = y * 2 + c

    def column(j, carry):
        at = pl.multiple_of(j * PAIR, PAIR)
        part = cols_v[pl.ds(at, PAIR)]
        scale = jnp.transpose(jnp.broadcast_to(scale_of(part), (PAIR, BLOCK)))[0:1]
        sums = [jnp.zeros((1, BLOCK), jnp.float32) for _ in range(2)]
        for i in range(row_owners):
            products = lax.dot_general(
                rows_v[i * PAIR : (i + 1) * PAIR],
                part,
                (((1,), (1,)), ((), ())),
                preferred_element_type=jnp.float32,
            )
            values = jnp.exp2(products * row_scales[i] * scale)
            for half in range(2):
                counts = weight[half, pl.ds(i, 1), pl.ds(at, PAIR)]
                for side in range(2):
                    block = values[half * BLOCK : (half + 1) * BLOCK, side * BLOCK : (side + 1) * BLOCK]
                    block = block * counts[:, side * BLOCK : (side + 1) * BLOCK]
                    block = block.astype(jnp.bfloat16)
                    w_v[
                        pl.ds(i * PAIR + half * BLOCK, BLOCK),
                        pl.ds(pl.multiple_of(at + side * BLOCK, BLOCK), BLOCK),
                    ] = block
                    sums[side] += jnp.sum(block.astype(jnp.float32), axis=0, keepdims=True)
        sums_out[:, pl.ds(at, PAIR)] = jnp.concatenate(sums, axis=1)

        @pl.when(j == own_col)
        def _():
            lanes = pl.ds(pl.multiple_of(at + xa * BLOCK, BLOCK), BLOCK)
            own_rows = pl.ds(pl.multiple_of(z * PAIR + xb * BLOCK, BLOCK), BLOCK)
            block = w_v[own_rows, lanes]
            w_v[own_rows, lanes] = jnp.where(eye, jnp.zeros_like(block), block)
            whole = w_v[:, lanes].astype(jnp.float32)
            sums_out[:, lanes] = jnp.sum(whole, axis=0, keepdims=True)

        out_copy(j).start()
        return carry

    lax.fori_loop(0, col_owners, column, 0)

    def drain(j, carry):
        out_copy(j).wait()
        return carry

    lax.fori_loop(0, col_owners, drain, 0)
    v_copy.wait()


def build_tile(row_pieces, col_pieces, ids, features, comps):
    y_count, z_count = lax.axis_size("y"), lax.axis_size("z")
    operands = []

    def slot_of(array):
        for slot, seen in enumerate(operands):
            if seen is array:
                return slot
        operands.append(array)
        return len(operands) - 1

    row_plan = [(slot_of(array), *rest) for array, *rest in row_pieces]
    col_plan = [(slot_of(array), *rest) for array, *rest in col_pieces]
    height, width = z_count * PAIR, 2 * y_count * PAIR
    copies = 2 * len(row_plan) + 3 * len(col_plan)
    kernel = functools.partial(
        tile_kernel, (len(operands), row_plan, col_plan), (y_count, z_count, features, comps)
    )
    return pl.pallas_call(
        kernel,
        out_shape=(
            jax.ShapeDtypeStruct((height, width), jnp.bfloat16),
            jax.ShapeDtypeStruct((1, width), jnp.float32),
            jax.ShapeDtypeStruct((width, comps), jnp.bfloat16),
        ),
        in_specs=[pl.BlockSpec(memory_space=pltpu.SMEM)]
        + [pl.BlockSpec(memory_space=pl.ANY)] * len(operands),
        out_specs=(
            pl.BlockSpec(memory_space=pl.ANY),
            pl.BlockSpec(memory_space=pltpu.VMEM),
            pl.BlockSpec(memory_space=pl.ANY),
        ),
        scratch_shapes=[
            pltpu.VMEM((height, features), jnp.bfloat16),
            pltpu.VMEM((width, features), jnp.bfloat16),
            pltpu.VMEM((width, comps), jnp.bfloat16),
            pltpu.VMEM((z_count, EXTRA, BLOCK), jnp.bfloat16),
            pltpu.VMEM((2 * y_count, EXTRA, BLOCK), jnp.bfloat16),
            pltpu.VMEM((2, z_count, width), jnp.float32),
            pltpu.VMEM((height, width), jnp.bfloat16),
            pltpu.SemaphoreType.DMA((copies,)),
            pltpu.SemaphoreType.DMA((2 * y_count + 1,)),
        ],
        compiler_params=pltpu.CompilerParams(vmem_limit_bytes=58 * 1024 * 1024),
        cost_estimate=pl.CostEstimate(
            flops=2 * height * width * features,
            bytes_accessed=2 * (height + width) * features + 2 * height * width,
            transcendentals=height * width,
        ),
        name="affinity_tile",
    )(ids, *operands)


def on_device(embed, start, links):
    slab_rows, features = embed.shape
    comps = start.shape[1]
    y_count, z_count = lax.axis_size("y"), lax.axis_size("z")
    y, z, c, xa, xb = (lax.axis_index(name) for name in ("y", "z", "c", "xa", "xb"))
    points = slab_rows * 2 * y_count * z_count
    highest = lax.Precision.HIGHEST

    note = jnp.pad(links.astype(jnp.bfloat16), ((0, EXTRA - 1), (0, BLOCK - links.shape[1])))
    row_own = lax.dynamic_slice_in_dim(embed, xa * PAIR, PAIR, 0)
    row_own = jnp.concatenate(
        [row_own, jnp.pad(note, ((0, 0), (0, features - BLOCK)))], axis=0
    )

    def blocks_of(values):
        shaped = values.reshape(2, 2, BLOCK, values.shape[1])
        return lax.dynamic_index_in_dim(shaped, xb, 1, keepdims=False).reshape(PAIR, -1)

    col_own = jnp.concatenate([blocks_of(embed), blocks_of(start)], axis=1)
    col_own = jnp.concatenate(
        [col_own, jnp.pad(note, ((0, 0), (0, features + comps - BLOCK)))], axis=0
    )
    row_pieces, col_pieces = exchange(row_own, col_own)
    ids = jnp.stack([y, z, c, xa, xb]).astype(jnp.int32)
    tile, sums, fetched_start = build_tile(row_pieces, col_pieces, ids, features, comps)

    inv_root_cols = lax.rsqrt(total_of(sums, COL_GROUP))[0]
    own_at = (y * 2 + c) * PAIR + xa * BLOCK
    inv_root = lax.dynamic_slice_in_dim(inv_root_cols, own_at, BLOCK, 0)[:, None]
    fetched = (fetched_start.astype(jnp.float32) * inv_root_cols[:, None]).astype(jnp.bfloat16)
    for turn in range(ITERS):
        part = jnp.dot(tile, fetched, preferred_element_type=jnp.float32).astype(jnp.bfloat16)
        parts = part.reshape(-1, BLOCK, comps)
        got = lax.all_to_all(parts, ROW_GROUP, split_axis=0, concat_axis=0, tiled=True)
        result = jnp.sum(got.astype(jnp.float32), axis=0) * inv_root
        gram = gram_total(jnp.dot(result.T, result, precision=highest))
        if turn == ITERS - 1:
            result = from_everyone(result, ("xa", "xb")).reshape(slab_rows, comps)
            return orthonormal(result, gram) * math.sqrt(points)
        current = orthonormal(result, gram)
        scaled = (current * inv_root).astype(jnp.bfloat16)
        fetched = from_everyone(scaled, COL_GROUP).reshape(-1, comps)


def solution(mesh):
    owners, reps = mesh.devices.shape
    side = math.isqrt(owners // 2)
    fine = Mesh(mesh.devices.reshape(side, side, 2, 2, reps // 2), ("y", "z", "c", "xa", "xb"))
    return jax.shard_map(
        on_device,
        mesh=fine,
        in_specs=(P(ROWS, None), P(ROWS, None), P(ROWS, None)),
        out_specs=P(ROWS, None),
        check_vma=False,
    )
```

```python
import functools
import math

import jax
import jax.numpy as jnp
from jax import lax
from jax.experimental import pallas as pl
from jax.experimental.pallas import tpu as pltpu
from jax.sharding import Mesh, PartitionSpec as P


BLOCK = 128
PAIR = 2 * BLOCK
EXTRA = 8
GROUP = 8
ITERS = 2
EPSILON = 1e-06
ROWS = ("y", "z", "c")
ROW_GROUP = ("z", "xb")
COL_GROUP = ("y", "c", "xa")


def from_everyone(shard, axes):
    copies = jnp.broadcast_to(shard, (lax.axis_size(axes), *shard.shape))
    return lax.all_to_all(copies, axes, split_axis=0, concat_axis=0, tiled=True)


def total_of(shard, axes):
    return jnp.sum(from_everyone(shard, axes), axis=0)


def gram_total(gram):
    wide = ("z", "xa", "xb")
    parts = gram.reshape(lax.axis_size(wide), -1, gram.shape[1])
    share = jnp.sum(lax.all_to_all(parts, wide, split_axis=0, concat_axis=0, tiled=True), axis=0)
    share = total_of(share, ("y", "c"))
    return from_everyone(share, wide).reshape(gram.shape)


def inverse_factor_kernel(gram_ref, out_ref):
    size = gram_ref.shape[0]
    count = size // GROUP
    diag = lax.broadcasted_iota(jnp.int32, (GROUP, size), 1) - lax.broadcasted_iota(
        jnp.int32, (GROUP, size), 0
    )
    sub = lax.broadcasted_iota(jnp.int32, (GROUP, size), 0)
    left = [gram_ref[g * GROUP : (g + 1) * GROUP] for g in range(count)]
    right = [(diag == g * GROUP).astype(jnp.float32) for g in range(count)]
    pivots = [None] * count

    def wide(column):
        return jnp.broadcast_to(column, (GROUP, size))

    def tall(row):
        return jnp.broadcast_to(row, (GROUP, size))

    for k in range(0, size, 2):
        home, at = divmod(k, GROUP)
        here = slice(at, at + 1)
        after = slice(at + 1, at + 2)
        first = [wide(left[g][:, k : k + 1]) for g in range(home, count)]
        second = [wide(left[g][:, k + 1 : k + 2]) for g in range(home, count)]
        a = tall(first[0][here])
        b = tall(first[0][after])
        d = tall(second[0][after])
        ratio = b / a
        rest = d - b * ratio
        inv_a, inv_rest = 1.0 / a, 1.0 / rest
        row_left, row_right = tall(left[home][here]), tall(right[home][here])
        next_left = tall(left[home][after]) - ratio * row_left
        next_right = tall(right[home][after]) - ratio * row_right
        for g in range(home, count):
            f = first[g - home] * inv_a
            h = (second[g - home] - first[g - home] * ratio) * inv_rest
            if g == home:
                mine = jnp.where(sub == at, a, jnp.where(sub == at + 1, rest, 0.0))
                pivots[g] = mine if pivots[g] is None else pivots[g] + mine
                f = jnp.where(sub > at, f, 0.0)
                h = jnp.where(sub > at + 1, h, 0.0)
            if g > home or at + 2 < GROUP:
                left[g] = left[g] - f * row_left - h * next_left
            right[g] = right[g] - f * row_right - h * next_right
    for g in range(count):
        out_ref[g * GROUP : (g + 1) * GROUP] = right[g] * lax.rsqrt(pivots[g])


def inverse_factor(gram):
    return pl.pallas_call(
        inverse_factor_kernel,
        out_shape=jax.ShapeDtypeStruct(gram.shape, jnp.float32),
        in_specs=[pl.BlockSpec(memory_space=pltpu.VMEM)],
        out_specs=pl.BlockSpec(memory_space=pltpu.VMEM),
        name="inverse_factor",
    )(gram)


def orthonormal(result, gram_matrix):
    inverse = inverse_factor(gram_matrix)
    return lax.dot_general(
        result, inverse, (((1,), (1,)), ((), ())), precision=lax.Precision.HIGHEST
    )


def exchange(row_own, col_own):
    size = lax.axis_size("z")
    assert size == lax.axis_size("y")
    onward = [(i, (i + 1) % size) for i in range(size)]
    backward = [(i, (i - 1) % size) for i in range(size)]
    height = row_own.shape[0]
    rows, cols = [], []

    def keep(place, first, piece):
        cols.append((piece, 0, place, first, False, piece.shape[0]))
        other = lax.ppermute(piece, "c", [(0, 1), (1, 0)])
        cols.append((other, 0, place, first, True, piece.shape[0]))

    rows.append((row_own, 0, 0, 0, height))
    keep(0, 0, col_own)
    row_a = row_b = row_own
    col_a = col_b = col_own
    for step in range(1, size // 2):
        col_a = lax.ppermute(col_a, "y", onward)
        col_b = lax.ppermute(col_b, "y", backward)
        row_a = lax.ppermute(row_a, "z", onward)
        row_b = lax.ppermute(row_b, "z", backward)
        rows.append((row_a, 0, size - step, 0, height))
        rows.append((row_b, 0, step, 0, height))
        keep(size - step, 0, col_a)
        keep(step, 0, col_b)
    far = size // 2
    col_top = lax.ppermute(col_a[:BLOCK], "y", onward)
    col_rest = lax.ppermute(col_b[BLOCK:], "y", backward)
    row_top = lax.ppermute(row_a[:BLOCK], "z", onward)
    row_rest = lax.ppermute(row_b[BLOCK:], "z", backward)
    rows.append((row_top, 0, far, 0, BLOCK))
    rows.append((row_rest, 0, far, BLOCK, height - BLOCK))
    keep(far, 0, col_top)
    keep(far, BLOCK, col_rest)
    return rows, cols


def tile_kernel(plan, sizes, ids, *refs):
    y_count, z_count, features, comps = sizes
    count, row_plan, col_plan = plan
    pieces, (w_out, sums_out, v_out) = refs[:count], refs[count : count + 3]
    rows_v, cols_v, start_v, row_links, col_links, weight, w_v, sems, out_sems = refs[count + 3 :]
    y, z, c, xa, xb = (ids[i] for i in range(5))
    row_owners, col_owners = z_count, 2 * y_count
    copies = []

    def copy(src, dst):
        made = pltpu.make_async_copy(src, dst, sems.at[len(copies)])
        made.start()
        copies.append(made)

    for slot, source, k, first, height in row_plan:
        ref = pieces[slot]
        owner = lax.rem(z + k, z_count)
        body = min(height, PAIR - first)
        at = pl.multiple_of(owner * PAIR + first, BLOCK)
        copy(ref.at[pl.ds(source, body)], rows_v.at[pl.ds(at, body)])
        if first + height > PAIR:
            copy(ref.at[pl.ds(source + body, EXTRA), pl.ds(0, BLOCK)], row_links.at[owner])
    for slot, source, k, first, other, height in col_plan:
        ref = pieces[slot]
        owner = lax.rem(y + k, y_count) * 2 + (1 - c if other else c)
        body = min(height, PAIR - first)
        at = pl.multiple_of(owner * PAIR + first, BLOCK)
        from_rows = pl.ds(source, body)
        copy(ref.at[from_rows, pl.ds(0, features)], cols_v.at[pl.ds(at, body)])
        copy(ref.at[from_rows, pl.ds(features, comps)], start_v.at[pl.ds(at, body)])
        if first + height > PAIR:
            copy(ref.at[pl.ds(source + body, EXTRA), pl.ds(0, BLOCK)], col_links.at[owner])
    for made in copies:
        made.wait()
    v_copy = pltpu.make_async_copy(start_v, v_out, out_sems.at[col_owners])
    v_copy.start()

    width = col_owners * PAIR
    lane = lax.broadcasted_iota(jnp.int32, (BLOCK, width), 1)
    place = lax.broadcasted_iota(jnp.int32, (BLOCK, width), 0)
    lane_owner = lane // PAIR
    lane_slab = ((lane_owner // 2) * z_count + z) * 2 + lane_owner % 2
    select = (place == lane_slab).astype(jnp.bfloat16)
    ahead_rows = jnp.concatenate([row_links[k][0:1] for k in range(row_owners)], axis=0)
    ahead = jnp.dot(ahead_rows, select, preferred_element_type=jnp.float32)
    spread_to = (place[:col_owners] == lane_owner[:col_owners]).astype(jnp.bfloat16)
    back_rows = jnp.concatenate([col_links[k][0:1] for k in range(col_owners)], axis=0)
    spread_back = lax.dot_general(
        back_rows, spread_to, (((0,), (0,)), ((), ())), preferred_element_type=jnp.float32
    ).astype(jnp.bfloat16)
    row_slab = (y * z_count + lax.broadcasted_iota(jnp.int32, (row_owners, BLOCK), 0)) * 2 + c
    row_pick = lax.broadcasted_iota(jnp.int32, (row_owners, BLOCK), 1) == row_slab
    back = jnp.dot(row_pick.astype(jnp.bfloat16), spread_back, preferred_element_type=jnp.float32)
    col_block = (xb + 2 * ((lane[:row_owners] // BLOCK) % 2)).astype(jnp.float32)
    same = (lane_owner[:row_owners] == y * 2 + c) & (place[:row_owners] == z)
    base = (ahead == col_block).astype(jnp.float32) + same.astype(jnp.float32)
    for half in range(2):
        row_block = (2 * xa + half).astype(jnp.float32)
        weight[half] = base + (back == row_block).astype(jnp.float32)

    factor = 2.0 / math.sqrt(features) * math.log2(math.e)

    def scale_of(values):
        wide = values.astype(jnp.float32)
        mean = jnp.sum(wide * wide, axis=-1, keepdims=True) * (1.0 / features)
        return lax.rsqrt(mean + EPSILON)

    row_scales = [
        scale_of(rows_v[pl.ds(i * PAIR, PAIR)]) * factor for i in range(row_owners)
    ]
    eye = lax.broadcasted_iota(jnp.int32, (BLOCK, BLOCK), 0) == lax.broadcasted_iota(
        jnp.int32, (BLOCK, BLOCK), 1
    )

    def out_copy(j):
        where = pl.ds(pl.multiple_of(j * PAIR, PAIR), PAIR)
        return pltpu.make_async_copy(w_v.at[:, where], w_out.at[:, where], out_sems.at[j])

    own_col = y * 2 + c

    def column(j, carry):
        at = pl.multiple_of(j * PAIR, PAIR)
        part = cols_v[pl.ds(at, PAIR)]
        scale = jnp.transpose(jnp.broadcast_to(scale_of(part), (PAIR, BLOCK)))[0:1]
        sums = [jnp.zeros((1, BLOCK), jnp.float32) for _ in range(2)]
        for i in range(row_owners):
            products = lax.dot_general(
                rows_v[i * PAIR : (i + 1) * PAIR],
                part,
                (((1,), (1,)), ((), ())),
                preferred_element_type=jnp.float32,
            )
            values = jnp.exp2(products * row_scales[i] * scale)
            for half in range(2):
                counts = weight[half, pl.ds(i, 1), pl.ds(at, PAIR)]
                for side in range(2):
                    block = values[half * BLOCK : (half + 1) * BLOCK, side * BLOCK : (side + 1) * BLOCK]
                    block = block * counts[:, side * BLOCK : (side + 1) * BLOCK]
                    block = block.astype(jnp.bfloat16)
                    w_v[
                        pl.ds(i * PAIR + half * BLOCK, BLOCK),
                        pl.ds(pl.multiple_of(at + side * BLOCK, BLOCK), BLOCK),
                    ] = block
                    sums[side] += jnp.sum(block.astype(jnp.float32), axis=0, keepdims=True)
        sums_out[:, pl.ds(at, PAIR)] = jnp.concatenate(sums, axis=1)

        @pl.when(j == own_col)
        def _():
            lanes = pl.ds(pl.multiple_of(at + xa * BLOCK, BLOCK), BLOCK)
            own_rows = pl.ds(pl.multiple_of(z * PAIR + xb * BLOCK, BLOCK), BLOCK)
            block = w_v[own_rows, lanes]
            w_v[own_rows, lanes] = jnp.where(eye, jnp.zeros_like(block), block)
            whole = w_v[:, lanes].astype(jnp.float32)
            sums_out[:, lanes] = jnp.sum(whole, axis=0, keepdims=True)

        out_copy(j).start()
        return carry

    lax.fori_loop(0, col_owners, column, 0)

    def drain(j, carry):
        out_copy(j).wait()
        return carry

    lax.fori_loop(0, col_owners, drain, 0)
    v_copy.wait()


def build_tile(row_pieces, col_pieces, ids, features, comps):
    y_count, z_count = lax.axis_size("y"), lax.axis_size("z")
    operands = []

    def slot_of(array):
        for slot, seen in enumerate(operands):
            if seen is array:
                return slot
        operands.append(array)
        return len(operands) - 1

    row_plan = [(slot_of(array), *rest) for array, *rest in row_pieces]
    col_plan = [(slot_of(array), *rest) for array, *rest in col_pieces]
    height, width = z_count * PAIR, 2 * y_count * PAIR
    copies = 2 * len(row_plan) + 3 * len(col_plan)
    kernel = functools.partial(
        tile_kernel, (len(operands), row_plan, col_plan), (y_count, z_count, features, comps)
    )
    return pl.pallas_call(
        kernel,
        out_shape=(
            jax.ShapeDtypeStruct((height, width), jnp.bfloat16),
            jax.ShapeDtypeStruct((1, width), jnp.float32),
            jax.ShapeDtypeStruct((width, comps), jnp.bfloat16),
        ),
        in_specs=[pl.BlockSpec(memory_space=pltpu.SMEM)]
        + [pl.BlockSpec(memory_space=pl.ANY)] * len(operands),
        out_specs=(
            pl.BlockSpec(memory_space=pl.ANY),
            pl.BlockSpec(memory_space=pltpu.VMEM),
            pl.BlockSpec(memory_space=pl.ANY),
        ),
        scratch_shapes=[
            pltpu.VMEM((height, features), jnp.bfloat16),
            pltpu.VMEM((width, features), jnp.bfloat16),
            pltpu.VMEM((width, comps), jnp.bfloat16),
            pltpu.VMEM((z_count, EXTRA, BLOCK), jnp.bfloat16),
            pltpu.VMEM((2 * y_count, EXTRA, BLOCK), jnp.bfloat16),
            pltpu.VMEM((2, z_count, width), jnp.float32),
            pltpu.VMEM((height, width), jnp.bfloat16),
            pltpu.SemaphoreType.DMA((copies,)),
            pltpu.SemaphoreType.DMA((2 * y_count + 1,)),
        ],
        compiler_params=pltpu.CompilerParams(vmem_limit_bytes=58 * 1024 * 1024),
        cost_estimate=pl.CostEstimate(
            flops=2 * height * width * features,
            bytes_accessed=2 * (height + width) * features + 2 * height * width,
            transcendentals=height * width,
        ),
        name="affinity_tile",
    )(ids, *operands)


def on_device(embed, start, links):
    slab_rows, features = embed.shape
    comps = start.shape[1]
    y_count, z_count = lax.axis_size("y"), lax.axis_size("z")
    y, z, c, xa, xb = (lax.axis_index(name) for name in ("y", "z", "c", "xa", "xb"))
    points = slab_rows * 2 * y_count * z_count
    highest = lax.Precision.HIGHEST

    note = jnp.pad(links.astype(jnp.bfloat16), ((0, EXTRA - 1), (0, BLOCK - links.shape[1])))
    row_own = lax.dynamic_slice_in_dim(embed, xa * PAIR, PAIR, 0)
    row_own = jnp.concatenate(
        [row_own, jnp.pad(note, ((0, 0), (0, features - BLOCK)))], axis=0
    )

    def blocks_of(values):
        shaped = values.reshape(2, 2, BLOCK, values.shape[1])
        return lax.dynamic_index_in_dim(shaped, xb, 1, keepdims=False).reshape(PAIR, -1)

    col_own = jnp.concatenate([blocks_of(embed), blocks_of(start)], axis=1)
    col_own = jnp.concatenate(
        [col_own, jnp.pad(note, ((0, 0), (0, features + comps - BLOCK)))], axis=0
    )
    row_pieces, col_pieces = exchange(row_own, col_own)
    ids = jnp.stack([y, z, c, xa, xb]).astype(jnp.int32)
    tile, sums, fetched_start = build_tile(row_pieces, col_pieces, ids, features, comps)

    sums = sums + lax.ppermute(sums, "xa", [(0, 1), (1, 0)])
    inv_root_cols = lax.rsqrt(total_of(sums, ("y", "c")))[0]
    own_at = (y * 2 + c) * PAIR + xa * BLOCK
    inv_root = lax.dynamic_slice_in_dim(inv_root_cols, own_at, BLOCK, 0)[:, None]
    fetched = (fetched_start.astype(jnp.float32) * inv_root_cols[:, None]).astype(jnp.bfloat16)
    for turn in range(ITERS):
        part = jnp.dot(tile, fetched, preferred_element_type=jnp.float32).astype(jnp.bfloat16)
        parts = part.reshape(-1, BLOCK, comps)
        got = lax.all_to_all(parts, ROW_GROUP, split_axis=0, concat_axis=0, tiled=True)
        result = jnp.sum(got.astype(jnp.float32), axis=0) * inv_root
        gram = gram_total(jnp.dot(result.T, result, precision=highest))
        if turn == ITERS - 1:
            result = from_everyone(result, ("xa", "xb")).reshape(slab_rows, comps)
            return orthonormal(result, gram) * math.sqrt(points)
        current = orthonormal(result, gram)
        scaled = (current * inv_root).astype(jnp.bfloat16)
        fetched = from_everyone(scaled, COL_GROUP).reshape(-1, comps)


def solution(mesh):
    owners, reps = mesh.devices.shape
    side = math.isqrt(owners // 2)
    fine = Mesh(mesh.devices.reshape(side, side, 2, 2, reps // 2), ("y", "z", "c", "xa", "xb"))
    return jax.shard_map(
        on_device,
        mesh=fine,
        in_specs=(P(ROWS, None), P(ROWS, None), P(ROWS, None)),
        out_specs=P(ROWS, None),
        check_vma=False,
    )
```

```python
import functools
import math

import jax
import jax.numpy as jnp
from jax import lax
from jax.experimental import pallas as pl
from jax.experimental.pallas import tpu as pltpu
from jax.sharding import Mesh, PartitionSpec as P


BLOCK = 128
PAIR = 2 * BLOCK
EXTRA = 8
GROUP = 8
ITERS = 2
EPSILON = 1e-06
ROWS = ("y", "z", "c")
ROW_GROUP = ("z", "xb")
COL_GROUP = ("y", "c", "xa")


def from_everyone(shard, axes):
    copies = jnp.broadcast_to(shard, (lax.axis_size(axes), *shard.shape))
    return lax.all_to_all(copies, axes, split_axis=0, concat_axis=0, tiled=True)


def total_of(shard, axes):
    return jnp.sum(from_everyone(shard, axes), axis=0)


def gram_total(gram):
    wide = ("z", "xa", "xb")
    parts = gram.reshape(lax.axis_size(wide), -1, gram.shape[1])
    share = jnp.sum(lax.all_to_all(parts, wide, split_axis=0, concat_axis=0, tiled=True), axis=0)
    share = total_of(share, ("y", "c"))
    return from_everyone(share, wide).reshape(gram.shape)


def inverse_factor_kernel(gram_ref, out_ref):
    size = gram_ref.shape[0]
    count = size // GROUP
    diag = lax.broadcasted_iota(jnp.int32, (GROUP, size), 1) - lax.broadcasted_iota(
        jnp.int32, (GROUP, size), 0
    )
    sub = lax.broadcasted_iota(jnp.int32, (GROUP, size), 0)
    left = [gram_ref[g * GROUP : (g + 1) * GROUP] for g in range(count)]
    right = [(diag == g * GROUP).astype(jnp.float32) for g in range(count)]
    pivots = [None] * count

    def wide(column):
        return jnp.broadcast_to(column, (GROUP, size))

    def tall(row):
        return jnp.broadcast_to(row, (GROUP, size))

    for k in range(0, size, 2):
        home, at = divmod(k, GROUP)
        here = slice(at, at + 1)
        after = slice(at + 1, at + 2)
        first = [wide(left[g][:, k : k + 1]) for g in range(home, count)]
        second = [wide(left[g][:, k + 1 : k + 2]) for g in range(home, count)]
        a = tall(first[0][here])
        b = tall(first[0][after])
        d = tall(second[0][after])
        ratio = b / a
        rest = d - b * ratio
        inv_a, inv_rest = 1.0 / a, 1.0 / rest
        row_left, row_right = tall(left[home][here]), tall(right[home][here])
        next_left = tall(left[home][after]) - ratio * row_left
        next_right = tall(right[home][after]) - ratio * row_right
        for g in range(home, count):
            f = first[g - home] * inv_a
            h = (second[g - home] - first[g - home] * ratio) * inv_rest
            if g == home:
                mine = jnp.where(sub == at, a, jnp.where(sub == at + 1, rest, 0.0))
                pivots[g] = mine if pivots[g] is None else pivots[g] + mine
                f = jnp.where(sub > at, f, 0.0)
                h = jnp.where(sub > at + 1, h, 0.0)
            if g > home or at + 2 < GROUP:
                left[g] = left[g] - f * row_left - h * next_left
            right[g] = right[g] - f * row_right - h * next_right
    for g in range(count):
        out_ref[g * GROUP : (g + 1) * GROUP] = right[g] * lax.rsqrt(pivots[g])


def inverse_factor(gram):
    return pl.pallas_call(
        inverse_factor_kernel,
        out_shape=jax.ShapeDtypeStruct(gram.shape, jnp.float32),
        in_specs=[pl.BlockSpec(memory_space=pltpu.VMEM)],
        out_specs=pl.BlockSpec(memory_space=pltpu.VMEM),
        name="inverse_factor",
    )(gram)


def orthonormal(result, gram_matrix):
    inverse = inverse_factor(gram_matrix)
    return lax.dot_general(
        result, inverse, (((1,), (1,)), ((), ())), precision=lax.Precision.HIGHEST
    )


def exchange(row_own, col_own):
    size = lax.axis_size("z")
    assert size == lax.axis_size("y")
    onward = [(i, (i + 1) % size) for i in range(size)]
    backward = [(i, (i - 1) % size) for i in range(size)]
    height = row_own.shape[0]
    rows, cols = [], []

    def keep(place, first, piece):
        cols.append((piece, 0, place, first, False, piece.shape[0]))
        other = lax.ppermute(piece, "c", [(0, 1), (1, 0)])
        cols.append((other, 0, place, first, True, piece.shape[0]))

    rows.append((row_own, 0, 0, 0, height))
    keep(0, 0, col_own)
    row_a = row_b = row_own
    col_a = col_b = col_own
    for step in range(1, size // 2):
        col_a = lax.ppermute(col_a, "y", onward)
        col_b = lax.ppermute(col_b, "y", backward)
        row_a = lax.ppermute(row_a, "z", onward)
        row_b = lax.ppermute(row_b, "z", backward)
        rows.append((row_a, 0, size - step, 0, height))
        rows.append((row_b, 0, step, 0, height))
        keep(size - step, 0, col_a)
        keep(step, 0, col_b)
    far = size // 2
    col_top = lax.ppermute(col_a[:BLOCK], "y", onward)
    col_rest = lax.ppermute(col_b[BLOCK:], "y", backward)
    row_top = lax.ppermute(row_a[:BLOCK], "z", onward)
    row_rest = lax.ppermute(row_b[BLOCK:], "z", backward)
    rows.append((row_top, 0, far, 0, BLOCK))
    rows.append((row_rest, 0, far, BLOCK, height - BLOCK))
    keep(far, 0, col_top)
    keep(far, BLOCK, col_rest)
    return rows, cols


def tile_kernel(plan, sizes, ids, *refs):
    y_count, z_count, features, comps = sizes
    count, row_plan, col_plan = plan
    pieces, (w_out, sums_out, v_out) = refs[:count], refs[count : count + 3]
    rows_v, cols_v, start_v, row_links, col_links, weight, w_v, sems, out_sems = refs[count + 3 :]
    y, z, c, xa, xb = (ids[i] for i in range(5))
    row_owners, col_owners = z_count, 2 * y_count
    copies, notes = [], []

    def copy(src, dst):
        made = pltpu.make_async_copy(src, dst, sems.at[len(copies)])
        made.start()
        copies.append(made)
        return made

    for slot, source, k, first, height in row_plan:
        ref = pieces[slot]
        owner = lax.rem(z + k, z_count)
        body = min(height, PAIR - first)
        at = pl.multiple_of(owner * PAIR + first, BLOCK)
        copy(ref.at[pl.ds(source, body)], rows_v.at[pl.ds(at, body)])
        if first + height > PAIR:
            notes.append(copy(ref.at[pl.ds(source + body, EXTRA), pl.ds(0, BLOCK)], row_links.at[owner]))
    for slot, source, k, first, other, height in col_plan:
        ref = pieces[slot]
        owner = lax.rem(y + k, y_count) * 2 + (1 - c if other else c)
        body = min(height, PAIR - first)
        at = pl.multiple_of(owner * PAIR + first, BLOCK)
        from_rows = pl.ds(source, body)
        copy(ref.at[from_rows, pl.ds(0, features)], cols_v.at[pl.ds(at, body)])
        copy(ref.at[from_rows, pl.ds(features, comps)], start_v.at[pl.ds(at, body)])
        if first + height > PAIR:
            notes.append(copy(ref.at[pl.ds(source + body, EXTRA), pl.ds(0, BLOCK)], col_links.at[owner]))
    for made in notes:
        made.wait()

    width = col_owners * PAIR
    lane = lax.broadcasted_iota(jnp.int32, (BLOCK, width), 1)
    place = lax.broadcasted_iota(jnp.int32, (BLOCK, width), 0)
    lane_owner = lane // PAIR
    lane_slab = ((lane_owner // 2) * z_count + z) * 2 + lane_owner % 2
    select = (place == lane_slab).astype(jnp.bfloat16)
    ahead_rows = jnp.concatenate([row_links[k][0:1] for k in range(row_owners)], axis=0)
    ahead = jnp.dot(ahead_rows, select, preferred_element_type=jnp.float32)
    spread_to = (place[:col_owners] == lane_owner[:col_owners]).astype(jnp.bfloat16)
    back_rows = jnp.concatenate([col_links[k][0:1] for k in range(col_owners)], axis=0)
    spread_back = lax.dot_general(
        back_rows, spread_to, (((0,), (0,)), ((), ())), preferred_element_type=jnp.float32
    ).astype(jnp.bfloat16)
    row_slab = (y * z_count + lax.broadcasted_iota(jnp.int32, (row_owners, BLOCK), 0)) * 2 + c
    row_pick = lax.broadcasted_iota(jnp.int32, (row_owners, BLOCK), 1) == row_slab
    back = jnp.dot(row_pick.astype(jnp.bfloat16), spread_back, preferred_element_type=jnp.float32)
    col_block = (xb + 2 * ((lane[:row_owners] // BLOCK) % 2)).astype(jnp.float32)
    same = (lane_owner[:row_owners] == y * 2 + c) & (place[:row_owners] == z)
    base = (ahead == col_block).astype(jnp.float32) + same.astype(jnp.float32)
    for half in range(2):
        row_block = (2 * xa + half).astype(jnp.float32)
        weight[half] = base + (back == row_block).astype(jnp.float32)

    for made in copies:
        if not any(made is note for note in notes):
            made.wait()
    v_copy = pltpu.make_async_copy(start_v, v_out, out_sems.at[col_owners])
    v_copy.start()
    factor = 2.0 / math.sqrt(features) * math.log2(math.e)

    def scale_of(values):
        wide = values.astype(jnp.float32)
        mean = jnp.sum(wide * wide, axis=-1, keepdims=True) * (1.0 / features)
        return lax.rsqrt(mean + EPSILON)

    row_scales = [
        scale_of(rows_v[pl.ds(i * PAIR, PAIR)]) * factor for i in range(row_owners)
    ]
    eye = lax.broadcasted_iota(jnp.int32, (BLOCK, BLOCK), 0) == lax.broadcasted_iota(
        jnp.int32, (BLOCK, BLOCK), 1
    )

    def out_copy(j):
        where = pl.ds(pl.multiple_of(j * PAIR, PAIR), PAIR)
        return pltpu.make_async_copy(w_v.at[:, where], w_out.at[:, where], out_sems.at[j])

    own_col = y * 2 + c

    def column(j, carry):
        at = pl.multiple_of(j * PAIR, PAIR)
        part = cols_v[pl.ds(at, PAIR)]
        scale = jnp.transpose(jnp.broadcast_to(scale_of(part), (PAIR, BLOCK)))[0:1]
        sums = [jnp.zeros((1, BLOCK), jnp.float32) for _ in range(2)]
        for i in range(row_owners):
            products = lax.dot_general(
                rows_v[i * PAIR : (i + 1) * PAIR],
                part,
                (((1,), (1,)), ((), ())),
                preferred_element_type=jnp.float32,
            )
            values = jnp.exp2(products * row_scales[i] * scale)
            for half in range(2):
                counts = weight[half, pl.ds(i, 1), pl.ds(at, PAIR)]
                for side in range(2):
                    block = values[half * BLOCK : (half + 1) * BLOCK, side * BLOCK : (side + 1) * BLOCK]
                    block = block * counts[:, side * BLOCK : (side + 1) * BLOCK]
                    block = block.astype(jnp.bfloat16)
                    w_v[
                        pl.ds(i * PAIR + half * BLOCK, BLOCK),
                        pl.ds(pl.multiple_of(at + side * BLOCK, BLOCK), BLOCK),
                    ] = block
                    sums[side] += jnp.sum(block.astype(jnp.float32), axis=0, keepdims=True)
        sums_out[:, pl.ds(at, PAIR)] = jnp.concatenate(sums, axis=1)

        @pl.when(j == own_col)
        def _():
            lanes = pl.ds(pl.multiple_of(at + xa * BLOCK, BLOCK), BLOCK)
            own_rows = pl.ds(pl.multiple_of(z * PAIR + xb * BLOCK, BLOCK), BLOCK)
            block = w_v[own_rows, lanes]
            w_v[own_rows, lanes] = jnp.where(eye, jnp.zeros_like(block), block)
            whole = w_v[:, lanes].astype(jnp.float32)
            sums_out[:, lanes] = jnp.sum(whole, axis=0, keepdims=True)

        out_copy(j).start()
        return carry

    lax.fori_loop(0, col_owners, column, 0)

    def drain(j, carry):
        out_copy(j).wait()
        return carry

    lax.fori_loop(0, col_owners, drain, 0)
    v_copy.wait()


def build_tile(row_pieces, col_pieces, ids, features, comps):
    y_count, z_count = lax.axis_size("y"), lax.axis_size("z")
    operands = []

    def slot_of(array):
        for slot, seen in enumerate(operands):
            if seen is array:
                return slot
        operands.append(array)
        return len(operands) - 1

    row_plan = [(slot_of(array), *rest) for array, *rest in row_pieces]
    col_plan = [(slot_of(array), *rest) for array, *rest in col_pieces]
    height, width = z_count * PAIR, 2 * y_count * PAIR
    copies = 2 * len(row_plan) + 3 * len(col_plan)
    kernel = functools.partial(
        tile_kernel, (len(operands), row_plan, col_plan), (y_count, z_count, features, comps)
    )
    return pl.pallas_call(
        kernel,
        out_shape=(
            jax.ShapeDtypeStruct((height, width), jnp.bfloat16),
            jax.ShapeDtypeStruct((1, width), jnp.float32),
            jax.ShapeDtypeStruct((width, comps), jnp.bfloat16),
        ),
        in_specs=[pl.BlockSpec(memory_space=pltpu.SMEM)]
        + [pl.BlockSpec(memory_space=pl.ANY)] * len(operands),
        out_specs=(
            pl.BlockSpec(memory_space=pl.ANY),
            pl.BlockSpec(memory_space=pltpu.VMEM),
            pl.BlockSpec(memory_space=pl.ANY),
        ),
        scratch_shapes=[
            pltpu.VMEM((height, features), jnp.bfloat16),
            pltpu.VMEM((width, features), jnp.bfloat16),
            pltpu.VMEM((width, comps), jnp.bfloat16),
            pltpu.VMEM((z_count, EXTRA, BLOCK), jnp.bfloat16),
            pltpu.VMEM((2 * y_count, EXTRA, BLOCK), jnp.bfloat16),
            pltpu.VMEM((2, z_count, width), jnp.float32),
            pltpu.VMEM((height, width), jnp.bfloat16),
            pltpu.SemaphoreType.DMA((copies,)),
            pltpu.SemaphoreType.DMA((2 * y_count + 1,)),
        ],
        compiler_params=pltpu.CompilerParams(vmem_limit_bytes=58 * 1024 * 1024),
        cost_estimate=pl.CostEstimate(
            flops=2 * height * width * features,
            bytes_accessed=2 * (height + width) * features + 2 * height * width,
            transcendentals=height * width,
        ),
        name="affinity_tile",
    )(ids, *operands)


def on_device(embed, start, links):
    slab_rows, features = embed.shape
    comps = start.shape[1]
    y_count, z_count = lax.axis_size("y"), lax.axis_size("z")
    y, z, c, xa, xb = (lax.axis_index(name) for name in ("y", "z", "c", "xa", "xb"))
    points = slab_rows * 2 * y_count * z_count
    highest = lax.Precision.HIGHEST

    note = jnp.pad(links.astype(jnp.bfloat16), ((0, EXTRA - 1), (0, BLOCK - links.shape[1])))
    row_own = lax.dynamic_slice_in_dim(embed, xa * PAIR, PAIR, 0)
    row_own = jnp.concatenate(
        [row_own, jnp.pad(note, ((0, 0), (0, features - BLOCK)))], axis=0
    )

    def blocks_of(values):
        shaped = values.reshape(2, 2, BLOCK, values.shape[1])
        return lax.dynamic_index_in_dim(shaped, xb, 1, keepdims=False).reshape(PAIR, -1)

    col_own = jnp.concatenate([blocks_of(embed), blocks_of(start)], axis=1)
    col_own = jnp.concatenate(
        [col_own, jnp.pad(note, ((0, 0), (0, features + comps - BLOCK)))], axis=0
    )
    row_pieces, col_pieces = exchange(row_own, col_own)
    ids = jnp.stack([y, z, c, xa, xb]).astype(jnp.int32)
    tile, sums, fetched_start = build_tile(row_pieces, col_pieces, ids, features, comps)

    sums = sums + lax.ppermute(sums, "xa", [(0, 1), (1, 0)])
    inv_root_cols = lax.rsqrt(total_of(sums, ("y", "c")))[0]
    own_at = (y * 2 + c) * PAIR + xa * BLOCK
    inv_root = lax.dynamic_slice_in_dim(inv_root_cols, own_at, BLOCK, 0)[:, None]
    fetched = (fetched_start.astype(jnp.float32) * inv_root_cols[:, None]).astype(jnp.bfloat16)
    for turn in range(ITERS):
        part = jnp.dot(tile, fetched, preferred_element_type=jnp.float32).astype(jnp.bfloat16)
        parts = part.reshape(-1, BLOCK, comps)
        got = lax.all_to_all(parts, ROW_GROUP, split_axis=0, concat_axis=0, tiled=True)
        result = jnp.sum(got.astype(jnp.float32), axis=0) * inv_root
        gram = gram_total(jnp.dot(result.T, result, precision=highest))
        if turn == ITERS - 1:
            result = from_everyone(result, ("xa", "xb")).reshape(slab_rows, comps)
            return orthonormal(result, gram) * math.sqrt(points)
        current = orthonormal(result, gram)
        scaled = (current * inv_root).astype(jnp.bfloat16)
        fetched = from_everyone(scaled, COL_GROUP).reshape(-1, comps)


def solution(mesh):
    owners, reps = mesh.devices.shape
    side = math.isqrt(owners // 2)
    fine = Mesh(mesh.devices.reshape(side, side, 2, 2, reps // 2), ("y", "z", "c", "xa", "xb"))
    return jax.shard_map(
        on_device,
        mesh=fine,
        in_specs=(P(ROWS, None), P(ROWS, None), P(ROWS, None)),
        out_specs=P(ROWS, None),
        check_vma=False,
    )
```
